8 devices in a mesh: data: 1 (over z), tp: 2 (over y), ep: 4 (over x, core).
Axes of the slice: x: 2, y: 2, z: 1, core: 2. Of those that a mesh axis runs over, the one named last changes fastest.
Arguments:
- tokens: bfloat16 [16384, 2048], P(('data', 'ep', 'tp'))
- expert_ids: int32 [16384, 4], P(('data', 'ep', 'tp'))
- gate_vals: float32 [16384, 4], P(('data', 'ep', 'tp'))
- slot_ids: int32 [16384, 4], P(('data', 'ep', 'tp'))
- send_counts: int32 [8, 60], P(('data', 'ep', 'tp'))
- shared_w1: bfloat16 [2048, 5632], P(None, 'tp')
- shared_w3: bfloat16 [2048, 5632], P(None, 'tp')
- shared_w2: bfloat16 [5632, 2048], P('tp')
- expert_w1: bfloat16 [60, 2048, 1408], P('ep')
- expert_w3: bfloat16 [60, 2048, 1408], P('ep')
- expert_w2: bfloat16 [60, 1408, 2048], P('ep')
Outputs:
- output: bfloat16 [16384, 2048], P(('data', 'ep', 'tp'))
All inputs are finite; a program needn't handle non-finite values.
Results may differ from the reference program's by a relative error of at most 0.00124.
Values are sent between devices in bfloat16 or wider.
A program may use at most 1.25 GiB of HBM per device.

```python
import jax
import jax.numpy as jnp
from jax import lax

EP = 4
TP = 2
TOKENS_DEV = 2048
D = 2048
FS = 5632
FF = 1408
EXPERTS = 60
TOP = 4
HOT = 7
CAP = 552

N_SRC = EP * TP
TOKENS = TOKENS_DEV * N_SRC


def draw_routing(route_key):
    key_hot, key_wts, key_perm = jax.random.split(route_key, 3)
    experts = jnp.arange(EXPERTS, dtype=jnp.int32)
    offset = jax.random.randint(key_hot, (), 0, EXPERTS, dtype=jnp.int32)
    is_hot = ((experts - offset) % EXPERTS) < HOT
    weights = jax.random.randint(key_wts, (N_SRC, EXPERTS), 1, 3, dtype=jnp.int32)
    cum_wts = jnp.cumsum(jnp.where(is_hot[None, :], 0, weights), axis=1)
    cold_total = TOKENS_DEV * TOP - HOT * CAP
    bounds = (cold_total * cum_wts) // cum_wts[:, -1:]
    prev_bounds = jnp.concatenate([jnp.zeros((N_SRC, 1), jnp.int32), bounds[:, :-1]], axis=1)
    counts = jnp.where(is_hot[None, :], CAP, bounds - prev_bounds).astype(jnp.int32)
    run_ends = jnp.cumsum(counts, axis=1)
    copy_pos = jnp.arange(TOKENS_DEV * TOP, dtype=jnp.int32)
    expert_of = jax.vmap(lambda end_row: jnp.searchsorted(end_row, copy_pos, side="right"))(run_ends).astype(jnp.int32)
    slot_of = copy_pos[None, :] - jnp.take_along_axis(run_ends - counts, expert_of, axis=1)
    expert_of = expert_of.reshape(N_SRC, TOP, TOKENS_DEV).transpose(0, 2, 1)
    slot_of = slot_of.reshape(N_SRC, TOP, TOKENS_DEV).transpose(0, 2, 1)
    tok_perms = jax.vmap(lambda perm_key: jax.random.permutation(perm_key, TOKENS_DEV))(jax.random.split(key_perm, N_SRC))
    expert_of = jnp.take_along_axis(expert_of, tok_perms[:, :, None], axis=1)
    slot_of = jnp.take_along_axis(slot_of, tok_perms[:, :, None], axis=1)
    return expert_of.reshape(TOKENS, TOP).astype(jnp.int32), slot_of.reshape(TOKENS, TOP).astype(jnp.int32), counts


def scaled_normal(weight_key, shape, fan_in):
    return (jax.random.normal(weight_key, shape, jnp.float32) * fan_in ** -0.5).astype(jnp.bfloat16)


def setup_inputs(seed: int = 0, part: int = 0) -> dict:
    base_key = jax.random.key(seed)
    part_key = jax.random.fold_in(base_key, part)
    key_x, key_gate, key_route = jax.random.split(part_key, 3)
    weight_keys = jax.random.split(jax.random.key(seed + 1), 6)
    tokens = jax.random.normal(key_x, (TOKENS, D), jnp.float32).astype(jnp.bfloat16)
    expert_ids, slot_ids, send_counts = draw_routing(key_route)
    gate_vals = jax.random.uniform(key_gate, (TOKENS, TOP), jnp.float32, 0.5, 1.5) * TOP ** -0.5
    return {
        "tokens": tokens,
        "expert_ids": expert_ids,
        "gate_vals": gate_vals,
        "slot_ids": slot_ids,
        "send_counts": send_counts,
        "shared_w1": scaled_normal(weight_keys[0], (D, FS), D),
        "shared_w3": scaled_normal(weight_keys[1], (D, FS), D),
        "shared_w2": scaled_normal(weight_keys[2], (FS, D), FS),
        "expert_w1": scaled_normal(weight_keys[3], (EXPERTS, D, FF), D),
        "expert_w3": scaled_normal(weight_keys[4], (EXPERTS, D, FF), D),
        "expert_w2": scaled_normal(weight_keys[5], (EXPERTS, FF, D), FF),
    }


def shared_block(tok_block, shared_w1, shared_w3, shared_w2):
    pre_gate = jnp.dot(tok_block, shared_w1, preferred_element_type=jnp.float32)
    pre_up = jnp.dot(tok_block, shared_w3, preferred_element_type=jnp.float32)
    hidden = (jax.nn.silu(pre_gate) * pre_up).astype(jnp.bfloat16)
    return jnp.dot(hidden, shared_w2, preferred_element_type=jnp.float32)


def reference(tokens, expert_ids, gate_vals, slot_ids, send_counts, shared_w1, shared_w3, shared_w2, expert_w1, expert_w3, expert_w2):
    tok_blocks = tokens.reshape(N_SRC, TOKENS_DEV, D)
    shared_out = lax.map(lambda tok_block: shared_block(tok_block, shared_w1, shared_w3, shared_w2), tok_blocks).reshape(TOKENS, D)
    src_ids = jnp.arange(TOKENS, dtype=jnp.int32) // TOKENS_DEV
    row_limit = send_counts[src_ids[:, None], expert_ids]
    kept_mask = (slot_ids >= 0) & (slot_ids < row_limit)
    n_rows = N_SRC * EXPERTS * CAP
    dest_row = jnp.where(kept_mask, (src_ids[:, None] * EXPERTS + expert_ids) * CAP + slot_ids, n_rows)
    copy_ids = jnp.arange(TOKENS * TOP, dtype=jnp.int32)
    owner_ids = jnp.full((n_rows,), TOKENS * TOP, jnp.int32).at[dest_row.reshape(-1)].set(copy_ids, mode="drop")
    owner_ids = owner_ids.reshape(N_SRC, EXPERTS, CAP).transpose(1, 0, 2).reshape(EXPERTS, N_SRC * CAP)
    flat_gates = gate_vals.reshape(-1)

    def expert_step(running, step_in):
        w_in, w_up, w_out, own_ids = step_in
        tok_of = own_ids // TOP
        expert_rows = jnp.take(tokens, tok_of, axis=0, mode="fill", fill_value=0)
        pre_gate = jnp.dot(expert_rows, w_in, preferred_element_type=jnp.float32)
        pre_up = jnp.dot(expert_rows, w_up, preferred_element_type=jnp.float32)
        hidden = (jax.nn.silu(pre_gate) * pre_up).astype(jnp.bfloat16)
        routed = jnp.dot(hidden, w_out, preferred_element_type=jnp.float32).astype(jnp.bfloat16)
        weight = jnp.take(flat_gates, own_ids, mode="fill", fill_value=0)
        running = running.at[tok_of].add(weight[:, None] * routed.astype(jnp.float32), mode="drop")
        return running, None

    routed_sum = lax.scan(expert_step, jnp.zeros((TOKENS, D), jnp.float32), (expert_w1, expert_w3, expert_w2, owner_ids))[0]
    return (tokens.astype(jnp.float32) + shared_out + routed_sum).astype(jnp.bfloat16)
```

```python
import functools

import jax
import jax.numpy as jnp
from jax import lax
from jax.experimental import pallas as pl
from jax.experimental.pallas import tpu as pltpu
from jax.sharding import PartitionSpec as P


CAP_FACTOR = 4
TILE = 256
UNROLL = 8
PAIR = 2
LANES = 128


def capacity_rows(n_tok, top_k, n_exp):
    return min(n_tok, ((CAP_FACTOR * n_tok * top_k // n_exp + 7) // 8) * 8)


def token_of(copy_id, top_k):
    return lax.div(copy_id, top_k) if top_k & (top_k - 1) else lax.shift_right_logical(copy_id, top_k.bit_length() - 1)


def segment(offs, expert, start, q):
    base = offs[expert * (PAIR + 1) + q]
    lo = jnp.maximum(base, start)
    hi = jnp.minimum(offs[expert * (PAIR + 1) + q + 1], start + TILE)
    return lo - start, jnp.maximum(hi - lo, 0), lo - base


def up_kernel(n_tok, top_k, n_local, table_cols, tile_exp, tile_row, offs, owner, x0, x1, w1_ref, w3_ref, u_ref, tok_vmem, rows_vmem, sems):
    step = pl.program_id(0)

    @pl.when(step == 0)
    def _():
        copies = [pltpu.make_async_copy(src, tok_vmem.at[pl.ds(q * n_tok, n_tok)], sems.at[q]) for q, src in enumerate((x0, x1))]
        for copy in copies:
            copy.start()
        for copy in copies:
            copy.wait()

    @pl.when(step < tile_row[pl.num_programs(0)])
    def _():
        expert, start = tile_exp[step], tile_row[step]
        for q in range(PAIR):
            dst, count, slot = segment(offs, expert, start, q)
            src = (q * n_local + expert) * table_cols + slot

            def gather(g, carry):
                rows = [tok_vmem[token_of(owner[src + g * UNROLL + j], top_k)] for j in range(UNROLL)]
                for j in range(UNROLL):
                    rows_vmem[dst + g * UNROLL + j] = rows[j]
                return carry

            lax.fori_loop(0, lax.div(count, UNROLL), gather, 0)

        rows = rows_vmem[...].reshape(TILE, -1)
        pre_gate = jnp.dot(rows, w1_ref[0], preferred_element_type=jnp.float32)
        pre_up = jnp.dot(rows, w3_ref[0], preferred_element_type=jnp.float32)
        u_ref[...] = (jax.nn.silu(pre_gate) * pre_up).astype(jnp.bfloat16)


def down_kernel(n_tok, top_k, n_local, table_cols, tile_exp, tile_row, offs, owner, gates, u_ref, w2_ref, *refs):
    *outs, acc, tile_vmem, sems = refs
    step = pl.program_id(0)
    cols = w2_ref.shape[2] // LANES

    @pl.when(step == 0)
    def _():
        def clear(g, carry):
            acc[pl.ds(g * 8, 8)] = jnp.zeros((8, cols, LANES), jnp.float32)
            return carry

        lax.fori_loop(0, PAIR * n_tok // 8, clear, 0)

    @pl.when(step < tile_row[pl.num_programs(0)])
    def _():
        out = jnp.dot(u_ref[...], w2_ref[0], preferred_element_type=jnp.float32).astype(jnp.bfloat16).astype(jnp.float32)
        for b in range(TILE // 8):
            for c in range(cols):
                tile_vmem[pl.ds(b * 8 * cols + c, 8, stride=cols), :] = out[b * 8 : (b + 1) * 8, c * LANES : (c + 1) * LANES]

        expert, start = tile_exp[step], tile_row[step]
        for q in range(PAIR):
            dst, count, slot = segment(offs, expert, start, q)
            src = (q * n_local + expert) * table_cols + slot

            def scatter(g, carry):
                copy_ids = [owner[src + g * UNROLL + j] for j in range(UNROLL)]
                toks = [token_of(copy_id, top_k) for copy_id in copy_ids]
                firsts = [pl.multiple_of((dst + g * UNROLL + j) * cols, cols) for j in range(UNROLL)]
                vals = [tile_vmem[pl.ds(firsts[j], cols), :] * gates[copy_ids[j]] for j in range(UNROLL)]
                olds = [acc[t] for t in toks]
                for j in range(UNROLL):
                    acc[toks[j]] = olds[j] + vals[j]
                return carry

            lax.fori_loop(0, lax.div(count, UNROLL), scatter, 0)

    @pl.when(step == pl.num_programs(0) - 1)
    def _():
        rows = PAIR * n_tok // len(outs)
        copies = [pltpu.make_async_copy(acc.at[pl.ds(i * rows, rows)], dst, sems.at[i]) for i, dst in enumerate(outs)]
        for copy in copies:
            copy.start()
        for copy in copies:
            copy.wait()


def solution(mesh):
    ep_size = mesh.shape["ep"]
    row_spec = P(("data", "ep", "tp"), None)
    expert_spec = P("ep", None, None)
    core_swap = [(r, r ^ 1) for r in range(ep_size)]
    chip_swap = [(r, r ^ 2) for r in range(ep_size)]

    def layer_body(tokens, expert_ids, gate_vals, slot_ids, send_counts, shared_w1, shared_w3, shared_w2, expert_w1, expert_w3, expert_w2):
        n_tok, d_model = tokens.shape
        top_k = expert_ids.shape[1]
        n_local, _, d_ff = expert_w1.shape
        n_exp = n_local * ep_size
        capacity = capacity_rows(n_tok, top_k, n_exp)
        table_cols = capacity + UNROLL
        max_tiles = n_local * PAIR * (capacity + UNROLL - 1) // TILE + n_local
        rank = lax.axis_index("ep")

        toks3 = tokens.reshape(n_tok, d_model // LANES, LANES)
        x_chip = lax.ppermute(toks3, "ep", chip_swap)
        x_core = lax.ppermute(toks3, "ep", core_swap)
        x_diag = lax.ppermute(x_chip, "ep", core_swap)
        peer_tokens = lax.ppermute(tokens, "tp", [(0, 1), (1, 0)])

        slots = jnp.where((slot_ids >= 0) & (slot_ids < capacity), slot_ids, table_cols)
        copy_ids = jnp.arange(n_tok * top_k, dtype=jnp.int32)
        dest = jnp.where(slots < capacity, expert_ids * table_cols + slots, n_exp * table_cols).reshape(-1)
        owner = jnp.zeros((n_exp * table_cols,), jnp.int32).at[dest].set(copy_ids, mode="drop").reshape(n_exp, table_cols)
        owner = jnp.concatenate([owner[:, :-1], send_counts[0][:, None]], axis=1)
        order = rank ^ jnp.arange(ep_size, dtype=jnp.int32)
        owner = lax.all_to_all(owner.reshape(ep_size, n_local, table_cols), "ep", 0, 0, tiled=True)
        owner = jnp.take(owner, order, axis=0)
        gates = lax.all_gather(gate_vals.reshape(-1), "ep", axis=0)
        gates = jnp.take(gates, order, axis=0)

        counts = jnp.minimum(owner[:, :, -1], capacity)

        any_spec = pl.BlockSpec(memory_space=pl.ANY)
        avg_rows = PAIR * n_tok * top_k // 2

        def plan(first):
            cnt = counts[first : first + PAIR]
            padded = (cnt + UNROLL - 1) // UNROLL * UNROLL
            offs = jnp.concatenate([jnp.zeros((1, n_local), jnp.int32), jnp.cumsum(padded, axis=0, dtype=jnp.int32)], axis=0)
            tiles = (offs[-1] + TILE - 1) // TILE
            ends = jnp.cumsum(tiles, dtype=jnp.int32)
            last = jnp.maximum(ends[-1], 1) - 1
            ids = jnp.minimum(jnp.arange(max_tiles, dtype=jnp.int32), last)
            past = ids[:, None] >= ends[None, :]
            tile_exp = jnp.minimum(jnp.sum(past, axis=1, dtype=jnp.int32), n_local - 1)
            tile_row = jnp.append((ids - jnp.sum(jnp.where(past, tiles[None, :], 0), axis=1, dtype=jnp.int32)) * TILE, last + 1)
            col = jnp.arange(table_cols, dtype=jnp.int32)
            base = jnp.arange(PAIR, dtype=jnp.int32)[:, None, None] * (n_tok * top_k)
            spare = PAIR * n_tok * top_k + (col % UNROLL) * top_k
            rows = jnp.where(col < cnt[:, :, None], owner[first : first + PAIR] + base, spare).reshape(-1)
            gate = jnp.append(gates[first : first + PAIR].reshape(-1), jnp.zeros((UNROLL * top_k,), jnp.float32))
            return tile_exp, tile_row, offs.T.reshape(-1), rows, gate

        def experts(planned, rows0, rows1, n_out):
            tile_exp, tile_row, offs, rows, gate = planned
            hidden = pl.pallas_call(
                functools.partial(up_kernel, n_tok, top_k, n_local, table_cols),
                grid_spec=pltpu.PrefetchScalarGridSpec(
                    num_scalar_prefetch=4,
                    grid=(max_tiles,),
                    in_specs=[any_spec] * PAIR + [pl.BlockSpec((1, d_model, d_ff), lambda i, te, tr, of, ow: (te[i], 0, 0))] * 2,
                    out_specs=pl.BlockSpec((TILE, d_ff), lambda i, te, tr, of, ow: (jnp.minimum(i, tr[max_tiles] - 1), 0)),
                    scratch_shapes=[
                        pltpu.VMEM((PAIR * n_tok + UNROLL, d_model // LANES, LANES), jnp.bfloat16),
                        pltpu.VMEM((TILE, d_model // LANES, LANES), jnp.bfloat16),
                        pltpu.SemaphoreType.DMA((PAIR,)),
                    ],
                ),
                out_shape=jax.ShapeDtypeStruct((max_tiles * TILE, d_ff), jnp.bfloat16),
                compiler_params=pltpu.CompilerParams(vmem_limit_bytes=60 * 2**20, dimension_semantics=("arbitrary",)),
                cost_estimate=pl.CostEstimate(flops=4 * avg_rows * d_model * d_ff, bytes_accessed=4 * n_local * d_model * d_ff, transcendentals=0),
                name="expert_up",
            )(tile_exp, tile_row, offs, rows, rows0, rows1, expert_w1, expert_w3)
            return pl.pallas_call(
                functools.partial(down_kernel, n_tok, top_k, n_local, table_cols),
                grid_spec=pltpu.PrefetchScalarGridSpec(
                    num_scalar_prefetch=5,
                    grid=(max_tiles,),
                    in_specs=[
                        pl.BlockSpec((TILE, d_ff), lambda i, te, tr, of, ow, ga: (jnp.minimum(i, tr[max_tiles] - 1), 0)),
                        pl.BlockSpec((1, d_ff, d_model), lambda i, te, tr, of, ow, ga: (te[i], 0, 0)),
                    ],
                    out_specs=[any_spec] * n_out,
                    scratch_shapes=[
                        pltpu.VMEM((PAIR * n_tok + UNROLL, d_model // LANES, LANES), jnp.float32),
                        pltpu.VMEM((TILE * d_model // LANES, LANES), jnp.float32),
                        pltpu.SemaphoreType.DMA((n_out,)),
                    ],
                ),
                out_shape=[jax.ShapeDtypeStruct((PAIR * n_tok // n_out, d_model // LANES, LANES), jnp.float32)] * n_out,
                compiler_params=pltpu.CompilerParams(vmem_limit_bytes=60 * 2**20, dimension_semantics=("arbitrary",)),
                cost_estimate=pl.CostEstimate(flops=2 * avg_rows * d_model * d_ff, bytes_accessed=2 * n_local * d_model * d_ff, transcendentals=0),
                name="expert_down",
            )(tile_exp, tile_row, offs, rows, gate, hidden, expert_w2)

        def shared_part(rows):
            pre_gate = jnp.dot(rows, shared_w1, preferred_element_type=jnp.float32)
            pre_up = jnp.dot(rows, shared_w3, preferred_element_type=jnp.float32)
            shared_hidden = (jax.nn.silu(pre_gate) * pre_up).astype(jnp.bfloat16)
            return jnp.dot(shared_hidden, shared_w2, preferred_element_type=jnp.float32)

        far_plan, near_plan = plan(PAIR), plan(0)
        own_part = shared_part(tokens)
        tile_exp, own_part = lax.optimization_barrier((far_plan[0], own_part))
        far_sums = experts((tile_exp, *far_plan[1:]), x_chip, x_diag, 4)
        peer_tokens, *far_sums = lax.optimization_barrier((peer_tokens, *far_sums))
        peer_rows = jnp.split(peer_tokens, 2)
        swapped = [lax.ppermute(part, "ep", core_swap) for part in far_sums[2:]]
        peer_0 = shared_part(peer_rows[0])
        swapped[0], peer_0 = lax.optimization_barrier((swapped[0], peer_0))
        chip_sums = [mine + theirs for mine, theirs in zip(far_sums[:2], swapped)]
        rows_1, *chip_sums = lax.optimization_barrier((peer_rows[1], *chip_sums))
        back = [lax.ppermute(part, "ep", chip_swap) for part in chip_sums]
        peer_1 = shared_part(rows_1)
        tile_exp, peer_1 = lax.optimization_barrier((near_plan[0], peer_1))
        peer_back = [lax.ppermute(part, "tp", [(0, 1), (1, 0)]) for part in (peer_0, peer_1)]
        own, core = experts((tile_exp, *near_plan[1:]), toks3, x_core, 2)
        near = (own + lax.ppermute(core, "ep", core_swap)).reshape(n_tok, d_model)
        kept = tokens.astype(jnp.float32) + own_part + near
        routed = jnp.concatenate([part.reshape(-1, d_model) for part in back])
        return (kept + jnp.concatenate(peer_back) + routed).astype(jnp.bfloat16)

    return jax.shard_map(
        layer_body,
        mesh=mesh,
        in_specs=(row_spec, row_spec, row_spec, row_spec, row_spec, P(None, "tp"), P(None, "tp"), P("tp", None), expert_spec, expert_spec, expert_spec),
        out_specs=row_spec,
        check_vma=False,
    )
```

```python
import functools

import jax
import jax.numpy as jnp
from jax import lax
from jax.experimental import pallas as pl
from jax.experimental.pallas import tpu as pltpu
from jax.sharding import PartitionSpec as P


CAP_FACTOR = 4
TILE = 256
UNROLL = 8
PAIR = 2
LANES = 128


def capacity_rows(n_tok, top_k, n_exp):
    return min(n_tok, ((CAP_FACTOR * n_tok * top_k // n_exp + 7) // 8) * 8)


def token_of(copy_id, top_k):
    return lax.div(copy_id, top_k) if top_k & (top_k - 1) else lax.shift_right_logical(copy_id, top_k.bit_length() - 1)


def segment(offs, expert, start, q):
    base = offs[expert * (PAIR + 1) + q]
    lo = jnp.maximum(base, start)
    hi = jnp.minimum(offs[expert * (PAIR + 1) + q + 1], start + TILE)
    return lo - start, jnp.maximum(hi - lo, 0), lo - base


def up_kernel(n_tok, top_k, n_local, table_cols, tile_exp, tile_row, offs, owner, *refs):
    *parts, w1_ref, w3_ref, u_ref, tok_vmem, rows_vmem, sems = refs
    step = pl.program_id(0)

    @pl.when(step == 0)
    def _():
        rows = PAIR * n_tok // len(parts)
        copies = [pltpu.make_async_copy(src, tok_vmem.at[pl.ds(i * rows, rows)], sems.at[i]) for i, src in enumerate(parts)]
        for copy in copies:
            copy.start()
        for copy in copies:
            copy.wait()

    @pl.when(step < tile_row[pl.num_programs(0)])
    def _():
        expert, start = tile_exp[step], tile_row[step]
        for q in range(PAIR):
            dst, count, slot = segment(offs, expert, start, q)
            src = (q * n_local + expert) * table_cols + slot

            def gather(g, carry):
                rows = [tok_vmem[token_of(owner[src + g * UNROLL + j], top_k)] for j in range(UNROLL)]
                for j in range(UNROLL):
                    rows_vmem[dst + g * UNROLL + j] = rows[j]
                return carry

            lax.fori_loop(0, lax.div(count, UNROLL), gather, 0)

        rows = rows_vmem[...].reshape(TILE, -1)
        pre_gate = jnp.dot(rows, w1_ref[0], preferred_element_type=jnp.float32)
        pre_up = jnp.dot(rows, w3_ref[0], preferred_element_type=jnp.float32)
        u_ref[...] = (jax.nn.silu(pre_gate) * pre_up).astype(jnp.bfloat16)


def down_kernel(n_tok, top_k, n_local, table_cols, tile_exp, tile_row, offs, owner, gates, u_ref, w2_ref, *refs):
    *outs, acc, tile_vmem, stage, sems = refs
    step = pl.program_id(0)
    cols = w2_ref.shape[2] // LANES

    @pl.when(step == 0)
    def _():
        def clear(g, carry):
            acc[pl.ds(pl.multiple_of(g * 128, 128), 128), :] = jnp.zeros((128, LANES), jnp.float32)
            return carry

        lax.fori_loop(0, PAIR * n_tok * cols // 128, clear, 0)

    @pl.when(step < tile_row[pl.num_programs(0)])
    def _():
        out = jnp.dot(u_ref[...], w2_ref[0], preferred_element_type=jnp.float32).astype(jnp.bfloat16).astype(jnp.float32)
        for b in range(TILE // 8):
            for c in range(cols):
                tile_vmem[pl.ds(b * 8 * cols + c, 8, stride=cols), :] = out[b * 8 : (b + 1) * 8, c * LANES : (c + 1) * LANES]

        expert, start = tile_exp[step], tile_row[step]
        for q in range(PAIR):
            dst, count, slot = segment(offs, expert, start, q)
            src = (q * n_local + expert) * table_cols + slot

            def scatter(g, carry):
                copy_ids = [owner[src + g * UNROLL + j] for j in range(UNROLL)]
                toks = [pl.ds(pl.multiple_of(token_of(copy_id, top_k) * cols, cols), cols) for copy_id in copy_ids]
                firsts = [pl.multiple_of((dst + g * UNROLL + j) * cols, cols) for j in range(UNROLL)]
                vals = [tile_vmem[pl.ds(firsts[j], cols), :] * gates[copy_ids[j]] for j in range(UNROLL)]
                olds = [acc[t, :] for t in toks]
                for j in range(UNROLL):
                    acc[toks[j], :] = olds[j] + vals[j]
                return carry

            lax.fori_loop(0, lax.div(count, UNROLL), scatter, 0)

    @pl.when(step == pl.num_programs(0) - 1)
    def _():
        rows = PAIR * n_tok // len(outs)
        block = stage.shape[1]
        for i, dst in enumerate(outs):

            def flush(g, carry):
                for half in range(2):
                    copy = pltpu.make_async_copy(stage.at[half], dst.at[pl.ds(pl.multiple_of((g * 2 + half) * block, block), block), :], sems.at[half])

                    @pl.when(g > 0)
                    def _():
                        copy.wait()

                    first = pl.multiple_of((i * rows + (g * 2 + half) * block) * cols, block * cols)
                    for b in range(block // 8):
                        for c in range(cols):
                            stage[half, b * 8 : (b + 1) * 8, c * LANES : (c + 1) * LANES] = acc[pl.ds(first + b * 8 * cols + c, 8, stride=cols), :]
                    copy.start()
                return carry

            lax.fori_loop(0, rows // (2 * block), flush, 0)
            for half in range(2):
                pltpu.make_async_copy(stage.at[half], dst.at[pl.ds(half * block, block), :], sems.at[half]).wait()


def solution(mesh):
    ep_size = mesh.shape["ep"]
    row_spec = P(("data", "ep", "tp"), None)
    expert_spec = P("ep", None, None)
    core_swap = [(r, r ^ 1) for r in range(ep_size)]
    chip_swap = [(r, r ^ 2) for r in range(ep_size)]

    def layer_body(tokens, expert_ids, gate_vals, slot_ids, send_counts, shared_w1, shared_w3, shared_w2, expert_w1, expert_w3, expert_w2):
        n_tok, d_model = tokens.shape
        top_k = expert_ids.shape[1]
        n_local, _, d_ff = expert_w1.shape
        n_exp = n_local * ep_size
        capacity = capacity_rows(n_tok, top_k, n_exp)
        table_cols = capacity + UNROLL
        max_tiles = n_local * PAIR * (capacity + UNROLL - 1) // TILE + n_local
        rank = lax.axis_index("ep")

        toks3 = tokens.reshape(n_tok, d_model // LANES, LANES)
        x_chip = lax.ppermute(toks3, "ep", chip_swap)
        peer_rows = [lax.ppermute(part, "tp", [(0, 1), (1, 0)]) for part in jnp.split(tokens, 2)]
        x_core = lax.ppermute(toks3, "ep", core_swap)
        x_diag = lax.ppermute(x_chip, "ep", core_swap)

        slots = jnp.where((slot_ids >= 0) & (slot_ids < capacity), slot_ids, table_cols)
        copy_ids = jnp.arange(n_tok * top_k, dtype=jnp.int32)
        dest = jnp.where(slots < capacity, expert_ids * table_cols + slots, n_exp * table_cols).reshape(-1)
        owner = jnp.zeros((n_exp * table_cols,), jnp.int32).at[dest].set(copy_ids, mode="drop").reshape(n_exp, table_cols)
        owner = jnp.concatenate([owner[:, :-1], send_counts[0][:, None]], axis=1).reshape(ep_size, n_local * table_cols)
        flat_gates = jnp.broadcast_to(gate_vals.reshape(1, -1), (ep_size, n_tok * top_k))
        message = jnp.concatenate([owner.astype(jnp.float32), flat_gates], axis=1)
        message = lax.all_to_all(message, "ep", 0, 0, tiled=True)
        message = jnp.take(message, rank ^ jnp.arange(ep_size, dtype=jnp.int32), axis=0)
        owner = message[:, : n_local * table_cols].astype(jnp.int32).reshape(ep_size, n_local, table_cols)
        gates = message[:, n_local * table_cols :]
        counts = jnp.minimum(owner[:, :, -1], capacity)

        any_spec = pl.BlockSpec(memory_space=pl.ANY)
        avg_rows = PAIR * n_tok * top_k // 2

        def plan(first):
            cnt = counts[first : first + PAIR]
            padded = (cnt + UNROLL - 1) // UNROLL * UNROLL
            offs = jnp.concatenate([jnp.zeros((1, n_local), jnp.int32), jnp.cumsum(padded, axis=0, dtype=jnp.int32)], axis=0)
            tiles = (offs[-1] + TILE - 1) // TILE
            ends = jnp.cumsum(tiles, dtype=jnp.int32)
            last = jnp.maximum(ends[-1], 1) - 1
            ids = jnp.minimum(jnp.arange(max_tiles, dtype=jnp.int32), last)
            past = ids[:, None] >= ends[None, :]
            tile_exp = jnp.minimum(jnp.sum(past, axis=1, dtype=jnp.int32), n_local - 1)
            tile_row = jnp.append((ids - jnp.sum(jnp.where(past, tiles[None, :], 0), axis=1, dtype=jnp.int32)) * TILE, last + 1)
            col = jnp.arange(table_cols, dtype=jnp.int32)
            base = jnp.arange(PAIR, dtype=jnp.int32)[:, None, None] * (n_tok * top_k)
            spare = PAIR * n_tok * top_k + (col % UNROLL) * top_k
            rows = jnp.where(col < cnt[:, :, None], owner[first : first + PAIR] + base, spare).reshape(-1)
            gate = jnp.append(gates[first : first + PAIR].reshape(-1), jnp.zeros((UNROLL * top_k,), jnp.float32))
            return tile_exp, tile_row, offs.T.reshape(-1), rows, gate

        def experts(planned, parts, n_out):
            tile_exp, tile_row, offs, rows, gate = planned
            hidden = pl.pallas_call(
                functools.partial(up_kernel, n_tok, top_k, n_local, table_cols),
                grid_spec=pltpu.PrefetchScalarGridSpec(
                    num_scalar_prefetch=4,
                    grid=(max_tiles,),
                    in_specs=[any_spec] * len(parts) + [pl.BlockSpec((1, d_model, d_ff), lambda i, te, tr, of, ow: (te[i], 0, 0))] * 2,
                    out_specs=pl.BlockSpec((TILE, d_ff), lambda i, te, tr, of, ow: (jnp.minimum(i, tr[max_tiles] - 1), 0)),
                    scratch_shapes=[
                        pltpu.VMEM((PAIR * n_tok + UNROLL, d_model // LANES, LANES), jnp.bfloat16),
                        pltpu.VMEM((TILE, d_model // LANES, LANES), jnp.bfloat16),
                        pltpu.SemaphoreType.DMA((len(parts),)),
                    ],
                ),
                out_shape=jax.ShapeDtypeStruct((max_tiles * TILE, d_ff), jnp.bfloat16),
                compiler_params=pltpu.CompilerParams(vmem_limit_bytes=60 * 2**20, dimension_semantics=("arbitrary",)),
                cost_estimate=pl.CostEstimate(flops=4 * avg_rows * d_model * d_ff, bytes_accessed=4 * n_local * d_model * d_ff, transcendentals=0),
                name="expert_up",
            )(tile_exp, tile_row, offs, rows, *parts, expert_w1, expert_w3)
            return pl.pallas_call(
                functools.partial(down_kernel, n_tok, top_k, n_local, table_cols),
                grid_spec=pltpu.PrefetchScalarGridSpec(
                    num_scalar_prefetch=5,
                    grid=(max_tiles,),
                    in_specs=[
                        pl.BlockSpec((TILE, d_ff), lambda i, te, tr, of, ow, ga: (jnp.minimum(i, tr[max_tiles] - 1), 0)),
                        pl.BlockSpec((1, d_ff, d_model), lambda i, te, tr, of, ow, ga: (te[i], 0, 0)),
                    ],
                    out_specs=[any_spec] * n_out,
                    scratch_shapes=[
                        pltpu.VMEM(((PAIR * n_tok + UNROLL) * d_model // LANES, LANES), jnp.float32),
                        pltpu.VMEM((TILE * d_model // LANES, LANES), jnp.float32),
                        pltpu.VMEM((2, min(64, n_tok // 4), d_model), jnp.float32),
                        pltpu.SemaphoreType.DMA((2,)),
                    ],
                ),
                out_shape=[jax.ShapeDtypeStruct((PAIR * n_tok // n_out, d_model), jnp.float32)] * n_out,
                compiler_params=pltpu.CompilerParams(vmem_limit_bytes=60 * 2**20, dimension_semantics=("arbitrary",)),
                cost_estimate=pl.CostEstimate(flops=2 * avg_rows * d_model * d_ff, bytes_accessed=2 * n_local * d_model * d_ff, transcendentals=0),
                name="expert_down",
            )(tile_exp, tile_row, offs, rows, gate, hidden, expert_w2)

        def shared_part(rows):
            pre_gate = jnp.dot(rows, shared_w1, preferred_element_type=jnp.float32)
            pre_up = jnp.dot(rows, shared_w3, preferred_element_type=jnp.float32)
            shared_hidden = (jax.nn.silu(pre_gate) * pre_up).astype(jnp.bfloat16)
            return jnp.dot(shared_hidden, shared_w2, preferred_element_type=jnp.float32)

        far_plan, near_plan = plan(PAIR), plan(0)
        own_part = shared_part(tokens)
        peer_rows[0], own_part = lax.optimization_barrier((peer_rows[0], own_part))
        peer_0 = shared_part(peer_rows[0])
        tile_exp, peer_0 = lax.optimization_barrier((far_plan[0], peer_0))
        far_sums = experts((tile_exp, *far_plan[1:]), (x_chip, x_diag), 4)
        peer_rows[1], *far_sums = lax.optimization_barrier((peer_rows[1], *far_sums))
        swapped = [lax.ppermute(part, "ep", core_swap) for part in far_sums[2:]]
        chip_sums = [mine + theirs for mine, theirs in zip(far_sums[:2], swapped)]
        peer_1 = shared_part(peer_rows[1])
        tile_exp, peer_1, *chip_sums = lax.optimization_barrier((near_plan[0], peer_1, *chip_sums))
        back = [lax.ppermute(part, "ep", chip_swap) for part in chip_sums]
        peer_back = [lax.ppermute(part, "tp", [(0, 1), (1, 0)]) for part in (peer_0, peer_1)]
        own, core = experts((tile_exp, *near_plan[1:]), (toks3, x_core), 2)
        near = own + lax.ppermute(core, "ep", core_swap)
        kept = tokens.astype(jnp.float32) + own_part + jnp.concatenate(peer_back) + near
        kept, *back = lax.optimization_barrier((kept, *back))
        return (kept + jnp.concatenate(back)).astype(jnp.bfloat16)

    return jax.shard_map(
        layer_body,
        mesh=mesh,
        in_specs=(row_spec, row_spec, row_spec, row_spec, row_spec, P(None, "tp"), P(None, "tp"), P("tp", None), expert_spec, expert_spec, expert_spec),
        out_specs=row_spec,
        check_vma=False,
    )
```

```python
import functools

import jax
import jax.numpy as jnp
from jax import lax
from jax.experimental import pallas as pl
from jax.experimental.pallas import tpu as pltpu
from jax.sharding import PartitionSpec as P


CAP_FACTOR = 4
TILE = 256
UNROLL = 8
LENT = 2
PAIR = 2
LANES = 128


def capacity_rows(n_tok, top_k, n_exp):
    return min(n_tok, ((CAP_FACTOR * n_tok * top_k // n_exp + 7) // 8) * 8)


def token_of(copy_id, top_k):
    return lax.div(copy_id, top_k) if top_k & (top_k - 1) else lax.shift_right_logical(copy_id, top_k.bit_length() - 1)


def segment(offs, expert, start, q):
    base = offs[expert * (PAIR + 1) + q]
    lo = jnp.maximum(base, start)
    hi = jnp.minimum(offs[expert * (PAIR + 1) + q + 1], start + TILE)
    return lo - start, jnp.maximum(hi - lo, 0), lo - base


def weights(step, tile_exp, tile_row, groups, n_exps, n_own, pairs, sems):
    expert = tile_exp[step]
    slot = groups[expert] & 1

    def fetch(e, slot):
        for i, (own, lent, buf) in enumerate(pairs):

            @pl.when(e < n_own)
            def _():
                pltpu.make_async_copy(own.at[e], buf.at[slot], sems.at[i, slot]).start()

            @pl.when(e >= n_own)
            def _():
                pltpu.make_async_copy(lent.at[e - n_own], buf.at[slot], sems.at[i, slot]).start()

    @pl.when(step == 0)
    def _():
        fetch(expert, slot)

    @pl.when(tile_row[step] == 0)
    def _():
        following = groups[n_exps + expert]

        @pl.when(following < n_exps)
        def _():
            fetch(following, 1 - slot)

        for i, (own, _, buf) in enumerate(pairs):
            pltpu.make_async_copy(own.at[0], buf.at[slot], sems.at[i, slot]).wait()

    return slot


def up_kernel(n_tok, top_k, n_local, n_exps, table_cols, tile_exp, tile_row, offs, groups, owner, *refs):
    *parts, w1, w3, lent1, lent3, u_ref, tok_vmem, rows_vmem, w1_vmem, w3_vmem, sems, w_sems = refs
    step = pl.program_id(0)

    @pl.when(step == 0)
    def _():
        rows = PAIR * n_tok // len(parts)
        copies = [pltpu.make_async_copy(src, tok_vmem.at[pl.ds(i * rows, rows)], sems.at[i]) for i, src in enumerate(parts)]
        for copy in copies:
            copy.start()
        for copy in copies:
            copy.wait()

    @pl.when(step < tile_row[pl.num_programs(0)])
    def _():
        w_slot = weights(step, tile_exp, tile_row, groups, n_exps, n_local, ((w1, lent1, w1_vmem), (w3, lent3, w3_vmem)), w_sems)
        expert, start = tile_exp[step], tile_row[step]
        for q in range(PAIR):
            dst, count, slot = segment(offs, expert, start, q)
            src = (q * n_exps + expert) * table_cols + slot

            def gather(g, carry):
                rows = [tok_vmem[token_of(owner[src + g * UNROLL + j], top_k)] for j in range(UNROLL)]
                for j in range(UNROLL):
                    rows_vmem[dst + g * UNROLL + j] = rows[j]
                return carry

            lax.fori_loop(0, lax.div(count, UNROLL), gather, 0)

        rows = rows_vmem[...].reshape(TILE, -1)
        pre_gate = jnp.dot(rows, w1_vmem[w_slot], preferred_element_type=jnp.float32)
        pre_up = jnp.dot(rows, w3_vmem[w_slot], preferred_element_type=jnp.float32)
        u_ref[...] = (jax.nn.silu(pre_gate) * pre_up).astype(jnp.bfloat16)


def down_kernel(n_tok, top_k, n_local, n_exps, table_cols, tile_exp, tile_row, offs, groups, owner, gates, u_ref, w2, lent2, *refs):
    *outs, acc, tile_vmem, w2_vmem, sems, w_sems = refs
    step = pl.program_id(0)
    cols = w2.shape[2] // LANES

    @pl.when(step == 0)
    def _():
        def clear(g, carry):
            acc[pl.ds(g * 8, 8)] = jnp.zeros((8, cols, LANES), jnp.float32)
            return carry

        lax.fori_loop(0, PAIR * n_tok // 8, clear, 0)

    @pl.when(step < tile_row[pl.num_programs(0)])
    def _():
        w_slot = weights(step, tile_exp, tile_row, groups, n_exps, n_local, ((w2, lent2, w2_vmem),), w_sems)
        out = jnp.dot(u_ref[...], w2_vmem[w_slot], preferred_element_type=jnp.float32).astype(jnp.bfloat16).astype(jnp.float32)
        for b in range(TILE // 8):
            for c in range(cols):
                tile_vmem[pl.ds(b * 8 * cols + c, 8, stride=cols), :] = out[b * 8 : (b + 1) * 8, c * LANES : (c + 1) * LANES]

        expert, start = tile_exp[step], tile_row[step]
        for q in range(PAIR):
            dst, count, slot = segment(offs, expert, start, q)
            src = (q * n_exps + expert) * table_cols + slot

            def scatter(g, carry):
                copy_ids = [owner[src + g * UNROLL + j] for j in range(UNROLL)]
                toks = [token_of(copy_id, top_k) for copy_id in copy_ids]
                firsts = [pl.multiple_of((dst + g * UNROLL + j) * cols, cols) for j in range(UNROLL)]
                vals = [tile_vmem[pl.ds(firsts[j], cols), :] * gates[copy_ids[j]] for j in range(UNROLL)]
                olds = [acc[t] for t in toks]
                for j in range(UNROLL):
                    acc[toks[j]] = olds[j] + vals[j]
                return carry

            lax.fori_loop(0, lax.div(count, UNROLL), scatter, 0)

    @pl.when(step == pl.num_programs(0) - 1)
    def _():
        rows = PAIR * n_tok // len(outs)
        copies = [
            pltpu.make_async_copy(acc.at[pl.ds(i * rows, rows), c, :], dst.at[:, pl.ds(c * LANES, LANES)], sems.at[i * cols + c])
            for i, dst in enumerate(outs)
            for c in range(cols)
        ]
        for copy in copies:
            copy.start()
        for copy in copies:
            copy.wait()


def lend_kernel(ids, *refs):
    for i in range(3):
        refs[3 + i][...] = refs[i][...]


def solution(mesh):
    ep_size = mesh.shape["ep"]
    row_spec = P(("data", "ep", "tp"), None)
    expert_spec = P("ep", None, None)
    core_swap = [(r, r ^ 1) for r in range(ep_size)]
    chip_swap = [(r, r ^ 2) for r in range(ep_size)]

    def layer_body(tokens, expert_ids, gate_vals, slot_ids, send_counts, shared_w1, shared_w3, shared_w2, expert_w1, expert_w3, expert_w2):
        n_tok, d_model = tokens.shape
        top_k = expert_ids.shape[1]
        n_local, _, d_ff = expert_w1.shape
        n_exp = n_local * ep_size
        capacity = capacity_rows(n_tok, top_k, n_exp)
        table_cols = capacity + UNROLL
        max_tiles = (n_local + LENT) * PAIR * (capacity + UNROLL - 1) // TILE + n_local + LENT
        rank = lax.axis_index("ep")

        toks3 = tokens.reshape(n_tok, d_model // LANES, LANES)
        x_chip = lax.ppermute(toks3, "ep", chip_swap)
        peer_rows = [lax.ppermute(part, "tp", [(0, 1), (1, 0)]) for part in jnp.split(tokens, 2)]
        x_core = lax.ppermute(toks3, "ep", core_swap)
        x_diag = lax.ppermute(x_chip, "ep", core_swap)

        slots = jnp.where((slot_ids >= 0) & (slot_ids < capacity), slot_ids, table_cols)
        copy_ids = jnp.arange(n_tok * top_k, dtype=jnp.int32)
        dest = jnp.where(slots < capacity, expert_ids * table_cols + slots, n_exp * table_cols).reshape(-1)
        owner = jnp.zeros((n_exp * table_cols,), jnp.int32).at[dest].set(copy_ids, mode="drop").reshape(n_exp, table_cols)
        owner = jnp.concatenate([owner[:, :-1], send_counts[0][:, None]], axis=1).reshape(ep_size, n_local * table_cols)
        flat_gates = jnp.broadcast_to(gate_vals.reshape(1, -1), (ep_size, n_tok * top_k))
        swapped_owner = owner.reshape(ep_size // 2, 2, -1)[:, ::-1].reshape(ep_size, -1)
        message = jnp.concatenate([owner.astype(jnp.float32), swapped_owner.astype(jnp.float32), flat_gates], axis=1)
        message = lax.all_to_all(message, "ep", 0, 0, tiled=True)
        message = jnp.take(message, rank ^ jnp.arange(ep_size, dtype=jnp.int32), axis=0)
        chip_owner = message[:, : 2 * n_local * table_cols].astype(jnp.int32).reshape(ep_size, 2 * n_local, table_cols)
        gates = message[:, 2 * n_local * table_cols :]
        chip_counts = jnp.minimum(chip_owner[:, :, -1], capacity)

        def largest(loads):
            found = []
            for _ in range(LENT):
                found.append(jnp.argmax(loads).astype(jnp.int32))
                loads = jnp.where(jnp.arange(n_local) == found[-1], -1, loads)
            return jnp.stack(found)

        lent = largest(lax.dynamic_slice_in_dim(jnp.minimum(send_counts[0], capacity), rank * n_local, n_local))
        w_arrays = (expert_w1, expert_w3, expert_w2)
        lend_in = [pl.BlockSpec((1, w.shape[1] // 2, w.shape[2]), lambda i, j, ids: (ids[i], j, 0)) for w in w_arrays]
        lend_out = [pl.BlockSpec((1, w.shape[1] // 2, w.shape[2]), lambda i, j, ids: (i, j, 0)) for w in w_arrays]
        lent_w = pl.pallas_call(
            lend_kernel,
            grid_spec=pltpu.PrefetchScalarGridSpec(num_scalar_prefetch=1, grid=(LENT, 2), in_specs=lend_in, out_specs=lend_out),
            out_shape=[jax.ShapeDtypeStruct((LENT, *w.shape[1:]), w.dtype) for w in w_arrays],
            compiler_params=pltpu.CompilerParams(vmem_limit_bytes=60 * 2**20),
            cost_estimate=pl.CostEstimate(flops=10**9, bytes_accessed=12 * LENT * d_model * d_ff, transcendentals=0),
            name="lend",
        )(lent, *w_arrays)
        got1, got3, got2 = [lax.ppermute(w, "ep", core_swap) for w in lent_w]

        sizes = jnp.sum(chip_counts, axis=0)
        borrowed = largest(chip_counts[1, n_local:])
        tiles_of = (sizes + TILE - 1) // TILE
        diff = jnp.sum(tiles_of[:n_local]) - jnp.sum(tiles_of[n_local:])
        give, take = [], []
        gap = diff
        for i in range(LENT):
            give.append(gap > tiles_of[lent[i]])
            gap = jnp.where(give[-1], gap - 2 * tiles_of[lent[i]], gap)
        gap = -diff
        for i in range(LENT):
            take.append(gap > tiles_of[n_local + borrowed[i]])
            gap = jnp.where(take[-1], gap - 2 * tiles_of[n_local + borrowed[i]], gap)
        given = sum(((jnp.arange(n_local) == lent[i]) & give[i]).astype(jnp.int32) for i in range(LENT)) > 0
        owner = jnp.concatenate([chip_owner[:, :n_local]] + [lax.dynamic_slice_in_dim(chip_owner, n_local + borrowed[i], 1, axis=1) for i in range(LENT)], axis=1)
        counts = jnp.minimum(owner[:, :, -1], capacity)
        active = jnp.concatenate([~given, jnp.stack(take)])
        counts = jnp.where(active[None, :], counts, 0)
        n_exps = n_local + LENT

        any_spec = pl.BlockSpec(memory_space=pl.ANY)
        avg_rows = PAIR * n_tok * top_k // 2

        def plan(first):
            cnt = counts[first : first + PAIR]
            padded = (cnt + UNROLL - 1) // UNROLL * UNROLL
            offs = jnp.concatenate([jnp.zeros((1, n_exps), jnp.int32), jnp.cumsum(padded, axis=0, dtype=jnp.int32)], axis=0)
            tiles = (offs[-1] + TILE - 1) // TILE
            ends = jnp.cumsum(tiles, dtype=jnp.int32)
            last = jnp.maximum(ends[-1], 1) - 1
            ids = jnp.minimum(jnp.arange(max_tiles, dtype=jnp.int32), last)
            past = ids[:, None] >= ends[None, :]
            tile_exp = jnp.minimum(jnp.sum(past, axis=1, dtype=jnp.int32), n_exps - 1)
            tile_row = jnp.append((ids - jnp.sum(jnp.where(past, tiles[None, :], 0), axis=1, dtype=jnp.int32)) * TILE, last + 1)
            used = tiles > 0
            exps = jnp.arange(n_exps, dtype=jnp.int32)
            later = (exps[None, :] > exps[:, None]) & used[None, :]
            following = jnp.min(jnp.where(later, exps[None, :], n_exps), axis=1)
            groups = jnp.append(jnp.cumsum(used, dtype=jnp.int32), following)
            col = jnp.arange(table_cols, dtype=jnp.int32)
            base = jnp.arange(PAIR, dtype=jnp.int32)[:, None, None] * (n_tok * top_k)
            spare = PAIR * n_tok * top_k + (col % UNROLL) * top_k
            rows = jnp.where(col < cnt[:, :, None], owner[first : first + PAIR] + base, spare).reshape(-1)
            gate = jnp.append(gates[first : first + PAIR].reshape(-1), jnp.zeros((UNROLL * top_k,), jnp.float32))
            return tile_exp, tile_row, offs.T.reshape(-1), groups, rows, gate

        def experts(planned, parts, n_out):
            tile_exp, tile_row, offs, groups, rows, gate = planned
            hidden = pl.pallas_call(
                functools.partial(up_kernel, n_tok, top_k, n_local, n_exps, table_cols),
                grid_spec=pltpu.PrefetchScalarGridSpec(
                    num_scalar_prefetch=5,
                    grid=(max_tiles,),
                    in_specs=[any_spec] * (len(parts) + 4),
                    out_specs=pl.BlockSpec((TILE, d_ff), lambda i, te, tr, of, gr, ow: (jnp.minimum(i, tr[max_tiles] - 1), 0)),
                    scratch_shapes=[
                        pltpu.VMEM((PAIR * n_tok + UNROLL, d_model // LANES, LANES), jnp.bfloat16),
                        pltpu.VMEM((TILE, d_model // LANES, LANES), jnp.bfloat16),
                        pltpu.VMEM((2, d_model, d_ff), jnp.bfloat16),
                        pltpu.VMEM((2, d_model, d_ff), jnp.bfloat16),
                        pltpu.SemaphoreType.DMA((len(parts),)),
                        pltpu.SemaphoreType.DMA((2, 2)),
                    ],
                ),
                out_shape=jax.ShapeDtypeStruct((max_tiles * TILE, d_ff), jnp.bfloat16),
                compiler_params=pltpu.CompilerParams(vmem_limit_bytes=60 * 2**20, dimension_semantics=("arbitrary",)),
                cost_estimate=pl.CostEstimate(flops=4 * avg_rows * d_model * d_ff, bytes_accessed=4 * n_local * d_model * d_ff, transcendentals=0),
                name="expert_up",
            )(tile_exp, tile_row, offs, groups, rows, *parts, expert_w1, expert_w3, got1, got3)
            return pl.pallas_call(
                functools.partial(down_kernel, n_tok, top_k, n_local, n_exps, table_cols),
                grid_spec=pltpu.PrefetchScalarGridSpec(
                    num_scalar_prefetch=6,
                    grid=(max_tiles,),
                    in_specs=[
                        pl.BlockSpec((TILE, d_ff), lambda i, te, tr, of, gr, ow, ga: (jnp.minimum(i, tr[max_tiles] - 1), 0)),
                        any_spec,
                        any_spec,
                    ],
                    out_specs=[any_spec] * n_out,
                    scratch_shapes=[
                        pltpu.VMEM((PAIR * n_tok + UNROLL, d_model // LANES, LANES), jnp.float32),
                        pltpu.VMEM((TILE * d_model // LANES, LANES), jnp.float32),
                        pltpu.VMEM((2, d_ff, d_model), jnp.bfloat16),
                        pltpu.SemaphoreType.DMA((n_out * d_model // LANES,)),
                        pltpu.SemaphoreType.DMA((1, 2)),
                    ],
                ),
                out_shape=[jax.ShapeDtypeStruct((PAIR * n_tok // n_out, d_model), jnp.float32)] * n_out,
                compiler_params=pltpu.CompilerParams(vmem_limit_bytes=60 * 2**20, dimension_semantics=("arbitrary",)),
                cost_estimate=pl.CostEstimate(flops=2 * avg_rows * d_model * d_ff, bytes_accessed=2 * n_local * d_model * d_ff, transcendentals=0),
                name="expert_down",
            )(tile_exp, tile_row, offs, groups, rows, gate, hidden, expert_w2, got2)

        def shared_part(rows):
            pre_gate = jnp.dot(rows, shared_w1, preferred_element_type=jnp.float32)
            pre_up = jnp.dot(rows, shared_w3, preferred_element_type=jnp.float32)
            shared_hidden = (jax.nn.silu(pre_gate) * pre_up).astype(jnp.bfloat16)
            return jnp.dot(shared_hidden, shared_w2, preferred_element_type=jnp.float32)

        far_plan, near_plan = plan(PAIR), plan(0)
        own_part = shared_part(tokens)
        peer_rows[0], own_part = lax.optimization_barrier((peer_rows[0], own_part))
        peer_0 = shared_part(peer_rows[0])
        tile_exp, peer_0 = lax.optimization_barrier((far_plan[0], peer_0))
        far_sums = experts((tile_exp, *far_plan[1:]), (x_chip, x_diag), 4)
        peer_rows[1], *far_sums = lax.optimization_barrier((peer_rows[1], *far_sums))
        swapped = [lax.ppermute(part, "ep", core_swap) for part in far_sums[2:]]
        chip_sums = [mine + theirs for mine, theirs in zip(far_sums[:2], swapped)]
        peer_1 = shared_part(peer_rows[1])
        tile_exp, peer_1, *chip_sums = lax.optimization_barrier((near_plan[0], peer_1, *chip_sums))
        back = [lax.ppermute(part, "ep", chip_swap) for part in chip_sums]
        peer_back = [lax.ppermute(part, "tp", [(0, 1), (1, 0)]) for part in (peer_0, peer_1)]
        own, core = experts((tile_exp, *near_plan[1:]), (toks3, x_core), 2)
        near = own + lax.ppermute(core, "ep", core_swap)
        kept = tokens.astype(jnp.float32) + own_part + jnp.concatenate(peer_back) + near
        kept, *back = lax.optimization_barrier((kept, *back))
        return (kept + jnp.concatenate(back)).astype(jnp.bfloat16)

    return jax.shard_map(
        layer_body,
        mesh=mesh,
        in_specs=(row_spec, row_spec, row_spec, row_spec, row_spec, P(None, "tp"), P(None, "tp"), P("tp", None), expert_spec, expert_spec, expert_spec),
        out_specs=row_spec,
        check_vma=False,
    )
```

```python
import functools

import jax
import jax.numpy as jnp
from jax import lax
from jax.experimental import pallas as pl
from jax.experimental.pallas import tpu as pltpu
from jax.sharding import PartitionSpec as P


CAP_FACTOR = 4
TILE = 256
UNROLL = 8
LENT = 3
PAIR = 2
LANES = 128


def capacity_rows(n_tok, top_k, n_exp):
    return min(n_tok, ((CAP_FACTOR * n_tok * top_k // n_exp + 7) // 8) * 8)


def token_of(copy_id, top_k):
    return lax.div(copy_id, top_k) if top_k & (top_k - 1) else lax.shift_right_logical(copy_id, top_k.bit_length() - 1)


def segment(offs, expert, start, q):
    base = offs[expert * (PAIR + 1) + q]
    lo = jnp.maximum(base, start)
    hi = jnp.minimum(offs[expert * (PAIR + 1) + q + 1], start + TILE)
    return lo - start, jnp.maximum(hi - lo, 0), lo - base


def weights(step, tile_exp, tile_row, groups, n_exps, n_own, pairs, sems):
    expert = tile_exp[step]
    slot = groups[expert] & 1

    def fetch(e, slot):
        for i, (own, lent, buf) in enumerate(pairs):

            @pl.when(e < n_own)
            def _():
                pltpu.make_async_copy(own.at[e], buf.at[slot], sems.at[i, slot]).start()

            @pl.when(e >= n_own)
            def _():
                pltpu.make_async_copy(lent.at[e - n_own], buf.at[slot], sems.at[i, slot]).start()

    @pl.when(step == 0)
    def _():
        fetch(expert, slot)

    @pl.when(tile_row[step] == 0)
    def _():
        following = groups[n_exps + expert]

        @pl.when(following < n_exps)
        def _():
            fetch(following, 1 - slot)

        for i, (own, _, buf) in enumerate(pairs):
            pltpu.make_async_copy(own.at[0], buf.at[slot], sems.at[i, slot]).wait()

    return slot


def up_kernel(n_tok, top_k, n_local, n_exps, table_cols, tile_exp, tile_row, offs, groups, owner, *refs):
    *parts, w1, w3, lent1, lent3, u_ref, tok_vmem, rows_vmem, w1_vmem, w3_vmem, sems, w_sems = refs
    step = pl.program_id(0)

    @pl.when(step == 0)
    def _():
        rows = PAIR * n_tok // len(parts)
        copies = [pltpu.make_async_copy(src, tok_vmem.at[pl.ds(i * rows, rows)], sems.at[i]) for i, src in enumerate(parts)]
        for copy in copies:
            copy.start()
        for copy in copies:
            copy.wait()

    @pl.when(step < tile_row[pl.num_programs(0)])
    def _():
        w_slot = weights(step, tile_exp, tile_row, groups, n_exps, n_local, ((w1, lent1, w1_vmem), (w3, lent3, w3_vmem)), w_sems)
        expert, start = tile_exp[step], tile_row[step]
        for q in range(PAIR):
            dst, count, slot = segment(offs, expert, start, q)
            src = (q * n_exps + expert) * table_cols + slot

            def gather(g, carry):
                rows = [tok_vmem[token_of(owner[src + g * UNROLL + j], top_k)] for j in range(UNROLL)]
                for j in range(UNROLL):
                    rows_vmem[dst + g * UNROLL + j] = rows[j]
                return carry

            lax.fori_loop(0, lax.div(count, UNROLL), gather, 0)

        rows = rows_vmem[...].reshape(TILE, -1)
        pre_gate = jnp.dot(rows, w1_vmem[w_slot], preferred_element_type=jnp.float32)
        pre_up = jnp.dot(rows, w3_vmem[w_slot], preferred_element_type=jnp.float32)
        u_ref[...] = (jax.nn.silu(pre_gate) * pre_up).astype(jnp.bfloat16)


def down_kernel(n_tok, top_k, n_local, n_exps, table_cols, tile_exp, tile_row, offs, groups, owner, gates, u_ref, w2, lent2, *refs):
    *outs, acc, tile_vmem, w2_vmem, sems, w_sems = refs
    step = pl.program_id(0)
    cols = w2.shape[2] // LANES

    @pl.when(step == 0)
    def _():
        def clear(g, carry):
            acc[pl.ds(g * 8, 8)] = jnp.zeros((8, cols, LANES), jnp.float32)
            return carry

        lax.fori_loop(0, PAIR * n_tok // 8, clear, 0)

    @pl.when(step < tile_row[pl.num_programs(0)])
    def _():
        w_slot = weights(step, tile_exp, tile_row, groups, n_exps, n_local, ((w2, lent2, w2_vmem),), w_sems)
        out = jnp.dot(u_ref[...], w2_vmem[w_slot], preferred_element_type=jnp.float32).astype(jnp.bfloat16).astype(jnp.float32)
        for b in range(TILE // 8):
            for c in range(cols):
                tile_vmem[pl.ds(b * 8 * cols + c, 8, stride=cols), :] = out[b * 8 : (b + 1) * 8, c * LANES : (c + 1) * LANES]

        expert, start = tile_exp[step], tile_row[step]
        for q in range(PAIR):
            dst, count, slot = segment(offs, expert, start, q)
            src = (q * n_exps + expert) * table_cols + slot

            def scatter(g, carry):
                copy_ids = [owner[src + g * UNROLL + j] for j in range(UNROLL)]
                toks = [token_of(copy_id, top_k) for copy_id in copy_ids]
                firsts = [pl.multiple_of((dst + g * UNROLL + j) * cols, cols) for j in range(UNROLL)]
                vals = [tile_vmem[pl.ds(firsts[j], cols), :] * gates[copy_ids[j]] for j in range(UNROLL)]
                olds = [acc[t] for t in toks]
                for j in range(UNROLL):
                    acc[toks[j]] = olds[j] + vals[j]
                return carry

            lax.fori_loop(0, lax.div(count, UNROLL), scatter, 0)

    @pl.when(step == pl.num_programs(0) - 1)
    def _():
        rows = PAIR * n_tok // len(outs)
        copies = [
            pltpu.make_async_copy(acc.at[pl.ds(i * rows, rows), c, :], dst.at[:, pl.ds(c * LANES, LANES)], sems.at[i * cols + c])
            for i, dst in enumerate(outs)
            for c in range(cols)
        ]
        for copy in copies:
            copy.start()
        for copy in copies:
            copy.wait()


def lend_kernel(ids, *refs):
    for i in range(3):
        refs[3 + i][...] = refs[i][...]


def solution(mesh):
    ep_size = mesh.shape["ep"]
    row_spec = P(("data", "ep", "tp"), None)
    expert_spec = P("ep", None, None)
    core_swap = [(r, r ^ 1) for r in range(ep_size)]
    chip_swap = [(r, r ^ 2) for r in range(ep_size)]

    def layer_body(tokens, expert_ids, gate_vals, slot_ids, send_counts, shared_w1, shared_w3, shared_w2, expert_w1, expert_w3, expert_w2):
        n_tok, d_model = tokens.shape
        top_k = expert_ids.shape[1]
        n_local, _, d_ff = expert_w1.shape
        n_exp = n_local * ep_size
        capacity = capacity_rows(n_tok, top_k, n_exp)
        table_cols = capacity + UNROLL
        max_tiles = (PAIR * n_tok * top_k + (n_local + LENT) * PAIR * (UNROLL - 1)) // TILE + n_local + LENT
        rank = lax.axis_index("ep")

        toks3 = tokens.reshape(n_tok, d_model // LANES, LANES)
        x_chip = lax.ppermute(toks3, "ep", chip_swap)
        peer_rows = [lax.ppermute(part, "tp", [(0, 1), (1, 0)]) for part in jnp.split(tokens, 2)]
        x_core = lax.ppermute(toks3, "ep", core_swap)
        x_diag = lax.ppermute(x_chip, "ep", core_swap)

        slots = jnp.where((slot_ids >= 0) & (slot_ids < capacity), slot_ids, table_cols)
        copy_ids = jnp.arange(n_tok * top_k, dtype=jnp.int32)
        dest = jnp.where(slots < capacity, expert_ids * table_cols + slots, n_exp * table_cols).reshape(-1)
        owner = jnp.zeros((n_exp * table_cols,), jnp.int32).at[dest].set(copy_ids, mode="drop").reshape(n_exp, table_cols)
        owner = jnp.concatenate([owner[:, :-1], send_counts[0][:, None]], axis=1).reshape(ep_size, n_local * table_cols)
        flat_gates = jnp.broadcast_to(gate_vals.reshape(1, -1), (ep_size, n_tok * top_k))
        swapped_owner = owner.reshape(ep_size // 2, 2, -1)[:, ::-1].reshape(ep_size, -1)
        message = jnp.concatenate([owner.astype(jnp.float32), swapped_owner.astype(jnp.float32), flat_gates], axis=1)
        message = lax.all_to_all(message, "ep", 0, 0, tiled=True)
        message = jnp.take(message, rank ^ jnp.arange(ep_size, dtype=jnp.int32), axis=0)
        chip_owner = message[:, : 2 * n_local * table_cols].astype(jnp.int32).reshape(ep_size, 2 * n_local, table_cols)
        gates = message[:, 2 * n_local * table_cols :]
        chip_counts = jnp.minimum(chip_owner[:, :, -1], capacity)

        def largest(loads):
            found = []
            for _ in range(LENT):
                found.append(jnp.argmax(loads).astype(jnp.int32))
                loads = jnp.where(jnp.arange(n_local) == found[-1], -1, loads)
            return jnp.stack(found)

        lent = largest(lax.dynamic_slice_in_dim(jnp.minimum(send_counts[0], capacity), rank * n_local, n_local))
        w_arrays = (expert_w1, expert_w3, expert_w2)
        lend_in = [pl.BlockSpec((1, w.shape[1] // 2, w.shape[2]), lambda i, j, ids: (ids[i], j, 0)) for w in w_arrays]
        lend_out = [pl.BlockSpec((1, w.shape[1] // 2, w.shape[2]), lambda i, j, ids: (i, j, 0)) for w in w_arrays]
        lent_w = pl.pallas_call(
            lend_kernel,
            grid_spec=pltpu.PrefetchScalarGridSpec(num_scalar_prefetch=1, grid=(LENT, 2), in_specs=lend_in, out_specs=lend_out),
            out_shape=[jax.ShapeDtypeStruct((LENT, *w.shape[1:]), w.dtype) for w in w_arrays],
            compiler_params=pltpu.CompilerParams(vmem_limit_bytes=60 * 2**20),
            cost_estimate=pl.CostEstimate(flops=10**9, bytes_accessed=12 * LENT * d_model * d_ff, transcendentals=0),
            name="lend",
        )(lent, *w_arrays)
        got1, got3, got2 = [lax.ppermute(w, "ep", core_swap) for w in lent_w]

        sizes = jnp.sum(chip_counts, axis=0)
        borrowed = largest(chip_counts[1, n_local:])
        tiles_of = (sizes + TILE - 1) // TILE
        diff = jnp.sum(tiles_of[:n_local]) - jnp.sum(tiles_of[n_local:])
        give, take = [], []
        gap = diff
        for i in range(LENT):
            give.append(gap > tiles_of[lent[i]])
            gap = jnp.where(give[-1], gap - 2 * tiles_of[lent[i]], gap)
        gap = -diff
        for i in range(LENT):
            take.append(gap > tiles_of[n_local + borrowed[i]])
            gap = jnp.where(take[-1], gap - 2 * tiles_of[n_local + borrowed[i]], gap)
        given = sum(((jnp.arange(n_local) == lent[i]) & give[i]).astype(jnp.int32) for i in range(LENT)) > 0
        owner = jnp.concatenate([chip_owner[:, :n_local]] + [lax.dynamic_slice_in_dim(chip_owner, n_local + borrowed[i], 1, axis=1) for i in range(LENT)], axis=1)
        counts = jnp.minimum(owner[:, :, -1], capacity)
        active = jnp.concatenate([~given, jnp.stack(take)])
        counts = jnp.where(active[None, :], counts, 0)
        n_exps = n_local + LENT

        any_spec = pl.BlockSpec(memory_space=pl.ANY)
        avg_rows = PAIR * n_tok * top_k // 2

        def plan(first):
            cnt = counts[first : first + PAIR]
            padded = (cnt + UNROLL - 1) // UNROLL * UNROLL
            offs = jnp.concatenate([jnp.zeros((1, n_exps), jnp.int32), jnp.cumsum(padded, axis=0, dtype=jnp.int32)], axis=0)
            tiles = (offs[-1] + TILE - 1) // TILE
            ends = jnp.cumsum(tiles, dtype=jnp.int32)
            last = jnp.maximum(ends[-1], 1) - 1
            ids = jnp.minimum(jnp.arange(max_tiles, dtype=jnp.int32), last)
            past = ids[:, None] >= ends[None, :]
            tile_exp = jnp.minimum(jnp.sum(past, axis=1, dtype=jnp.int32), n_exps - 1)
            tile_row = jnp.append((ids - jnp.sum(jnp.where(past, tiles[None, :], 0), axis=1, dtype=jnp.int32)) * TILE, last + 1)
            used = tiles > 0
            exps = jnp.arange(n_exps, dtype=jnp.int32)
            later = (exps[None, :] > exps[:, None]) & used[None, :]
            following = jnp.min(jnp.where(later, exps[None, :], n_exps), axis=1)
            groups = jnp.append(jnp.cumsum(used, dtype=jnp.int32), following)
            col = jnp.arange(table_cols, dtype=jnp.int32)
            base = jnp.arange(PAIR, dtype=jnp.int32)[:, None, None] * (n_tok * top_k)
            spare = PAIR * n_tok * top_k + (col % UNROLL) * top_k
            rows = jnp.where(col < cnt[:, :, None], owner[first : first + PAIR] + base, spare).reshape(-1)
            gate = jnp.append(gates[first : first + PAIR].reshape(-1), jnp.zeros((UNROLL * top_k,), jnp.float32))
            return tile_exp, tile_row, offs.T.reshape(-1), groups, rows, gate

        def experts(planned, parts, n_out):
            tile_exp, tile_row, offs, groups, rows, gate = planned
            hidden = pl.pallas_call(
                functools.partial(up_kernel, n_tok, top_k, n_local, n_exps, table_cols),
                grid_spec=pltpu.PrefetchScalarGridSpec(
                    num_scalar_prefetch=5,
                    grid=(max_tiles,),
                    in_specs=[any_spec] * (len(parts) + 4),
                    out_specs=pl.BlockSpec((TILE, d_ff), lambda i, te, tr, of, gr, ow: (jnp.minimum(i, tr[max_tiles] - 1), 0)),
                    scratch_shapes=[
                        pltpu.VMEM((PAIR * n_tok + UNROLL, d_model // LANES, LANES), jnp.bfloat16),
                        pltpu.VMEM((TILE, d_model // LANES, LANES), jnp.bfloat16),
                        pltpu.VMEM((2, d_model, d_ff), jnp.bfloat16),
                        pltpu.VMEM((2, d_model, d_ff), jnp.bfloat16),
                        pltpu.SemaphoreType.DMA((len(parts),)),
                        pltpu.SemaphoreType.DMA((2, 2)),
                    ],
                ),
                out_shape=jax.ShapeDtypeStruct((max_tiles * TILE, d_ff), jnp.bfloat16),
                compiler_params=pltpu.CompilerParams(vmem_limit_bytes=60 * 2**20, dimension_semantics=("arbitrary",)),
                cost_estimate=pl.CostEstimate(flops=4 * avg_rows * d_model * d_ff, bytes_accessed=4 * n_local * d_model * d_ff, transcendentals=0),
                name="expert_up",
            )(tile_exp, tile_row, offs, groups, rows, *parts, expert_w1, expert_w3, got1, got3)
            return pl.pallas_call(
                functools.partial(down_kernel, n_tok, top_k, n_local, n_exps, table_cols),
                grid_spec=pltpu.PrefetchScalarGridSpec(
                    num_scalar_prefetch=6,
                    grid=(max_tiles,),
                    in_specs=[
                        pl.BlockSpec((TILE, d_ff), lambda i, te, tr, of, gr, ow, ga: (jnp.minimum(i, tr[max_tiles] - 1), 0)),
                        any_spec,
                        any_spec,
                    ],
                    out_specs=[any_spec] * n_out,
                    scratch_shapes=[
                        pltpu.VMEM((PAIR * n_tok + UNROLL, d_model // LANES, LANES), jnp.float32),
                        pltpu.VMEM((TILE * d_model // LANES, LANES), jnp.float32),
                        pltpu.VMEM((2, d_ff, d_model), jnp.bfloat16),
                        pltpu.SemaphoreType.DMA((n_out * d_model // LANES,)),
                        pltpu.SemaphoreType.DMA((1, 2)),
                    ],
                ),
                out_shape=[jax.ShapeDtypeStruct((PAIR * n_tok // n_out, d_model), jnp.float32)] * n_out,
                compiler_params=pltpu.CompilerParams(vmem_limit_bytes=60 * 2**20, dimension_semantics=("arbitrary",)),
                cost_estimate=pl.CostEstimate(flops=2 * avg_rows * d_model * d_ff, bytes_accessed=2 * n_local * d_model * d_ff, transcendentals=0),
                name="expert_down",
            )(tile_exp, tile_row, offs, groups, rows, gate, hidden, expert_w2, got2)

        def shared_part(rows):
            pre_gate = jnp.dot(rows, shared_w1, preferred_element_type=jnp.float32)
            pre_up = jnp.dot(rows, shared_w3, preferred_element_type=jnp.float32)
            shared_hidden = (jax.nn.silu(pre_gate) * pre_up).astype(jnp.bfloat16)
            return jnp.dot(shared_hidden, shared_w2, preferred_element_type=jnp.float32)

        far_plan, near_plan = plan(PAIR), plan(0)
        own_part = shared_part(tokens)
        peer_rows[0], own_part = lax.optimization_barrier((peer_rows[0], own_part))
        peer_0 = shared_part(peer_rows[0])
        tile_exp, peer_0 = lax.optimization_barrier((far_plan[0], peer_0))
        far_sums = experts((tile_exp, *far_plan[1:]), (x_chip, x_diag), 4)
        peer_rows[1], *far_sums = lax.optimization_barrier((peer_rows[1], *far_sums))
        swapped = [lax.ppermute(part, "ep", core_swap) for part in far_sums[2:]]
        chip_sums = [mine + theirs for mine, theirs in zip(far_sums[:2], swapped)]
        peer_1 = shared_part(peer_rows[1])
        tile_exp, peer_1 = lax.optimization_barrier((near_plan[0], peer_1))
        back = [lax.ppermute(part, "ep", chip_swap) for part in chip_sums]
        peer_back = [lax.ppermute(part, "tp", [(0, 1), (1, 0)]) for part in (peer_0, peer_1)]
        own, core = experts((tile_exp, *near_plan[1:]), (toks3, x_core), 2)
        core = lax.ppermute(core, "ep", core_swap)
        kept = lax.optimization_barrier(tokens.astype(jnp.float32) + own_part + jnp.concatenate(peer_back) + own)
        return (kept + core + jnp.concatenate(back)).astype(jnp.bfloat16)

    return jax.shard_map(
        layer_body,
        mesh=mesh,
        in_specs=(row_spec, row_spec, row_spec, row_spec, row_spec, P(None, "tp"), P(None, "tp"), P("tp", None), expert_spec, expert_spec, expert_spec),
        out_specs=row_spec,
        check_vma=False,
    )
```
